64 devices in a mesh: dp: 4 (over x, y), cp: 16 (over z, core).
Axes of the slice: x: 2, y: 2, z: 8, core: 2. Of those that a mesh axis runs over, the one named last changes fastest.
The devices are a block of a 4x4x8 slice.
Arguments:
- x_tokens: bfloat16 [32, 8192, 640], P('dp', 'cp'), parts along dimension 0
- dy_tokens: bfloat16 [32, 8192, 640], P('dp', 'cp'), parts along dimension 0
- positions: int32 [32, 8192], P('dp', 'cp'), parts along dimension 0
- w_query: bfloat16 [640, 1024], replicated
- w_key: bfloat16 [640, 256], replicated
- w_value: bfloat16 [640, 256], replicated
- w_out: bfloat16 [1024, 640], replicated
- w_gate: bfloat16 [640, 2048], replicated
- w_up: bfloat16 [640, 2048], replicated
- w_down: bfloat16 [2048, 640], replicated
- g_attn_in: bfloat16 [640], replicated
- g_attn_out: bfloat16 [640], replicated
- g_mlp_in: bfloat16 [640], replicated
- g_mlp_out: bfloat16 [640], replicated
- g_query: bfloat16 [256], replicated
- g_key: bfloat16 [256], replicated
Outputs:
- output 1: bfloat16 [32, 8192, 640], P('dp', 'cp'), parts along dimension 0
- output 2: bfloat16 [32, 8192, 640], P('dp', 'cp'), parts along dimension 0
- output 3: bfloat16 [2560, 1024], P('dp'), parts along dimension 0
- output 4: bfloat16 [2560, 256], P('dp'), parts along dimension 0
- output 5: bfloat16 [2560, 256], P('dp'), parts along dimension 0
- output 6: bfloat16 [4096, 640], P('dp'), parts along dimension 0
- output 7: bfloat16 [2560, 2048], P('dp'), parts along dimension 0
- output 8: bfloat16 [2560, 2048], P('dp'), parts along dimension 0
- output 9: bfloat16 [8192, 640], P('dp'), parts along dimension 0
- output 10: bfloat16 [2560], P('dp'), parts along dimension 0
- output 11: bfloat16 [2560], P('dp'), parts along dimension 0
- output 12: bfloat16 [2560], P('dp'), parts along dimension 0
- output 13: bfloat16 [2560], P('dp'), parts along dimension 0
- output 14: bfloat16 [1024], P('dp'), parts along dimension 0
- output 15: bfloat16 [1024], P('dp'), parts along dimension 0
There are 4 independent parts. The reference program is written for one: setup_inputs(seed, part) draws one part's arguments, and reference() takes and returns one part's arrays. A program takes and returns all parts, laid end to end along the dimension named above; an argument that names none is the same for every part.
All inputs are finite; a program needn't handle non-finite values.
Results may differ from the reference program's by a relative error of at most 0.02.
Values are sent between devices in bfloat16 or wider.
A program may use at most 768 MiB of HBM per device.

```python
import jax
import jax.numpy as jnp
from jax import lax

BATCH = 8
SEQ_LEN = 8192
MODEL_DIM = 640
HEADS = 4
KV_HEADS = 1
HEAD_DIM = 256
FFN_DIM = 2048
WINDOW = 512
QUERY_SCALAR = 256
GROUPS = HEADS // KV_HEADS
BLOCKS = SEQ_LEN // WINDOW
SCORE_SCALE = QUERY_SCALAR ** -0.5
NORM_EPS = 1e-6
ROPE_BASE = 10000.0


def draw_matrix(rng_key, fan_in, fan_out):
    return (jax.random.normal(rng_key, (fan_in, fan_out), jnp.float32) * fan_in ** -0.5).astype(jnp.bfloat16)


def draw_gain(rng_key, vec_width):
    return (0.3 * jax.random.normal(rng_key, (vec_width,), jnp.float32)).astype(jnp.bfloat16)


def setup_inputs(seed: int = 0, part: int = 0) -> dict:
    base_key = jax.random.key(seed)
    part_key = jax.random.fold_in(base_key, part)
    data_keys = jax.random.split(part_key, 4)
    weight_keys = jax.random.split(base_key, 13)
    x_tokens = jax.random.normal(data_keys[0], (BATCH, SEQ_LEN, MODEL_DIM), jnp.float32).astype(jnp.bfloat16)
    dy_tokens = jax.random.normal(data_keys[1], (BATCH, SEQ_LEN, MODEL_DIM), jnp.float32).astype(jnp.bfloat16)
    start_pos = jax.random.randint(data_keys[2], (BATCH, 1), 0, 1024, jnp.int32)
    pos_steps = jax.random.randint(data_keys[3], (BATCH, SEQ_LEN), 1, 3, jnp.int32)
    positions = (start_pos + jnp.cumsum(pos_steps, axis=1)).astype(jnp.int32)
    q_width = HEADS * HEAD_DIM
    kv_width = KV_HEADS * HEAD_DIM
    return {
        "x_tokens": x_tokens,
        "dy_tokens": dy_tokens,
        "positions": positions,
        "w_query": draw_matrix(weight_keys[0], MODEL_DIM, q_width),
        "w_key": draw_matrix(weight_keys[1], MODEL_DIM, kv_width),
        "w_value": draw_matrix(weight_keys[2], MODEL_DIM, kv_width),
        "w_out": draw_matrix(weight_keys[3], q_width, MODEL_DIM),
        "w_gate": draw_matrix(weight_keys[4], MODEL_DIM, FFN_DIM),
        "w_up": draw_matrix(weight_keys[5], MODEL_DIM, FFN_DIM),
        "w_down": draw_matrix(weight_keys[6], FFN_DIM, MODEL_DIM),
        "g_attn_in": draw_gain(weight_keys[7], MODEL_DIM),
        "g_attn_out": draw_gain(weight_keys[8], MODEL_DIM),
        "g_mlp_in": draw_gain(weight_keys[9], MODEL_DIM),
        "g_mlp_out": draw_gain(weight_keys[10], MODEL_DIM),
        "g_query": draw_gain(weight_keys[11], HEAD_DIM),
        "g_key": draw_gain(weight_keys[12], HEAD_DIM),
    }


def rms_scale(values, gain_vec):
    mean_sq = jnp.mean(values * values, axis=-1, keepdims=True)
    return values * lax.rsqrt(mean_sq + NORM_EPS) * (1.0 + gain_vec.astype(jnp.float32))


def rope_tables(pos_seq):
    half_dim = HEAD_DIM // 2
    inv_freq = ROPE_BASE ** (-2.0 * jnp.arange(half_dim, dtype=jnp.float32) / HEAD_DIM)
    angles = pos_seq.astype(jnp.float32)[:, None] * inv_freq[None, :]
    return jnp.cos(angles), jnp.sin(angles)


def head_prep(proj_vals, gain_vec, cos_tab, sin_tab):
    normed = rms_scale(proj_vals, gain_vec)
    half_dim = HEAD_DIM // 2
    first_half = normed[..., :half_dim]
    second_half = normed[..., half_dim:]
    cos_part = cos_tab[:, None, :]
    sin_part = sin_tab[:, None, :]
    return jnp.concatenate([first_half * cos_part - second_half * sin_part, second_half * cos_part + first_half * sin_part], axis=-1)


def window_keys(flat_seq):
    blocked = flat_seq.reshape((BLOCKS + 1, WINDOW) + flat_seq.shape[1:])
    return jnp.concatenate([blocked[:-1], blocked[1:]], axis=1)


def local_attention(q_rot, k_rot, v_val, pos_seq):
    kv_pad = jnp.zeros((WINDOW, KV_HEADS, HEAD_DIM), jnp.float32)
    k_win = window_keys(jnp.concatenate([kv_pad, k_rot.astype(jnp.float32)], axis=0))
    v_win = window_keys(jnp.concatenate([kv_pad, v_val.astype(jnp.float32)], axis=0))
    pos_win = window_keys(jnp.concatenate([jnp.zeros((WINDOW,), jnp.int32), pos_seq], axis=0))
    ext_index = jnp.arange(BLOCKS)[:, None] * WINDOW + jnp.arange(2 * WINDOW)[None, :]
    q_pos = pos_seq.reshape(BLOCKS, WINDOW)[:, :, None]
    visible = (ext_index >= WINDOW)[:, None, :] & (pos_win[:, None, :] > q_pos - WINDOW) & (pos_win[:, None, :] <= q_pos)
    q_blk = q_rot.astype(jnp.float32).reshape(BLOCKS, WINDOW, KV_HEADS, GROUPS, HEAD_DIM)
    scores = jnp.einsum("nqkgd,nskd->nkgqs", q_blk, k_win) * SCORE_SCALE
    scores = jnp.where(visible[:, None, None], scores, -1e30)
    prob_vals = jax.nn.softmax(scores, axis=-1).astype(jnp.bfloat16).astype(jnp.float32)
    attn_vals = jnp.einsum("nkgqs,nskd->nqkgd", prob_vals, v_win)
    return attn_vals.reshape(SEQ_LEN, HEADS * HEAD_DIM).astype(jnp.bfloat16)


def layer_forward(x_seq, pos_seq, weights):
    (w_query, w_key, w_value, w_out, w_gate, w_up, w_down,
     g_attn_in, g_attn_out, g_mlp_in, g_mlp_out, g_query, g_key) = weights
    x_f32 = x_seq.astype(jnp.float32)
    h_attn = rms_scale(x_f32, g_attn_in).astype(jnp.bfloat16)
    cos_tab, sin_tab = rope_tables(pos_seq)
    q_proj = jnp.dot(h_attn, w_query.astype(jnp.bfloat16), preferred_element_type=jnp.float32)
    k_proj = jnp.dot(h_attn, w_key.astype(jnp.bfloat16), preferred_element_type=jnp.float32)
    v_val = jnp.dot(h_attn, w_value.astype(jnp.bfloat16), preferred_element_type=jnp.float32).astype(jnp.bfloat16).reshape(SEQ_LEN, KV_HEADS, HEAD_DIM)
    q_rot = head_prep(q_proj.reshape(SEQ_LEN, HEADS, HEAD_DIM), g_query, cos_tab, sin_tab).astype(jnp.bfloat16)
    k_rot = head_prep(k_proj.reshape(SEQ_LEN, KV_HEADS, HEAD_DIM), g_key, cos_tab, sin_tab).astype(jnp.bfloat16)
    attn_out = local_attention(q_rot, k_rot, v_val, pos_seq)
    o_proj = jnp.dot(attn_out, w_out.astype(jnp.bfloat16), preferred_element_type=jnp.float32)
    x_mid32 = (x_f32 + rms_scale(o_proj, g_attn_out)).astype(jnp.bfloat16).astype(jnp.float32)
    h_mlp = rms_scale(x_mid32, g_mlp_in).astype(jnp.bfloat16)
    gate_proj = jnp.dot(h_mlp, w_gate.astype(jnp.bfloat16), preferred_element_type=jnp.float32)
    up_proj = jnp.dot(h_mlp, w_up.astype(jnp.bfloat16), preferred_element_type=jnp.float32)
    hidden_act = (jax.nn.gelu(gate_proj, approximate=True) * up_proj).astype(jnp.bfloat16)
    down_proj = jnp.dot(hidden_act, w_down.astype(jnp.bfloat16), preferred_element_type=jnp.float32)
    return (x_mid32 + rms_scale(down_proj, g_mlp_out)).astype(jnp.bfloat16)


def reference(x_tokens, dy_tokens, positions, w_query, w_key, w_value, w_out, w_gate, w_up, w_down, g_attn_in, g_attn_out, g_mlp_in, g_mlp_out, g_query, g_key):
    weights = tuple(item.astype(jnp.float32) for item in (w_query, w_key, w_value, w_out, w_gate, w_up, w_down, g_attn_in, g_attn_out, g_mlp_in, g_mlp_out, g_query, g_key))
    grad_init = tuple(jnp.zeros(item.shape, jnp.float32) for item in weights)

    def scan_step(grad_acc, seq_inputs):
        x_seq, dy_seq, pos_seq = seq_inputs

        def forward_fn(x_arg, w_arg):
            return layer_forward(x_arg, pos_seq, w_arg)

        y_seq, back_fn = jax.vjp(forward_fn, x_seq, weights)
        dx_seq, dw_seq = back_fn(dy_seq)
        new_acc = tuple(left + right for left, right in zip(grad_acc, dw_seq))
        return new_acc, (y_seq, dx_seq)

    grads, (y_tokens, dx_tokens) = lax.scan(scan_step, grad_init, (x_tokens, dy_tokens, positions))
    (dw_query, dw_key, dw_value, dw_out, dw_gate, dw_up, dw_down,
     dg_attn_in, dg_attn_out, dg_mlp_in, dg_mlp_out, dg_query, dg_key) = grads
    return (y_tokens, dx_tokens, dw_query.astype(jnp.bfloat16), dw_key.astype(jnp.bfloat16), dw_value.astype(jnp.bfloat16), dw_out.astype(jnp.bfloat16), dw_gate.astype(jnp.bfloat16), dw_up.astype(jnp.bfloat16), dw_down.astype(jnp.bfloat16), dg_attn_in.astype(jnp.bfloat16), dg_attn_out.astype(jnp.bfloat16), dg_mlp_in.astype(jnp.bfloat16), dg_mlp_out.astype(jnp.bfloat16), dg_query.astype(jnp.bfloat16), dg_key.astype(jnp.bfloat16))
```

```python
import functools
import jax
import jax.numpy as jnp
from jax import lax
from jax.experimental import pallas as pl
from jax.experimental.pallas import tpu as pltpu
from jax.sharding import PartitionSpec as P

NORM_EPS = 1e-6
ROPE_BASE = 10000.0
NEG = -1e30
F32 = jnp.float32
BF16 = jnp.bfloat16
VMEM_CAP = 67000000
MESH = pl.DeviceIdType.MESH


def window_size(model_dim):
    return 512 * min(2, 1 + model_dim // 2048)


def score_scale(model_dim, num_heads, head_dim):
    scalar = 256 if head_dim == 256 else model_dim // num_heads
    return scalar ** -0.5


def dot(a, b):
    return jnp.dot(a, b, preferred_element_type=F32)


def dot_nt(a, b):
    return lax.dot_general(a, b, (((1,), (1,)), ((), ())), preferred_element_type=F32)


def unit(v):
    r = lax.rsqrt(jnp.mean(v * v, axis=-1, keepdims=True) + NORM_EPS)
    return v * r, r


def unit_back(n, r, t):
    return r * (t - n * jnp.mean(t * n, axis=-1, keepdims=True))


def rope(n, cos, sin):
    half = n.shape[-1] // 2
    a, b = n[:, :half], n[:, half:]
    return jnp.concatenate([a * cos - b * sin, b * cos + a * sin], axis=-1)


def rope_back(d, cos, sin):
    half = d.shape[-1] // 2
    a, b = d[:, :half], d[:, half:]
    return jnp.concatenate([a * cos + b * sin, b * cos - a * sin], axis=-1)


def gain(ref):
    return 1.0 + ref[...].astype(F32)


def colsum(v):
    return jnp.sum(v, axis=0, keepdims=True)


def kv_kernel(x_ref, cos_ref, sin_ref, wkv_ref, g_in_ref, g_k_ref, kv_ref):
    head = g_k_ref.shape[1]
    n, _ = unit(x_ref[0].astype(F32))
    h = (n * gain(g_in_ref)).astype(BF16)
    proj = dot(h, wkv_ref[...])
    kn, _ = unit(proj[:, :head])
    k = rope(kn * gain(g_k_ref), cos_ref[0], sin_ref[0])
    kv_ref[0, :, :head] = k.astype(BF16)
    kv_ref[0, :, head:] = proj[:, head:].astype(BF16)


def visible_bias(pos_ref, pos_col, first, keys, queries, window, tokens):
    key_pos = pos_col[first:first + keys]
    query_pos = pos_ref[0, :, tokens + first:tokens + first + queries]
    seen = (key_pos > query_pos - window) & (key_pos <= query_pos)
    return jnp.where(seen, 0.0, NEG).astype(F32)


def column_of(row):
    return jnp.transpose(jnp.broadcast_to(row, (8, row.shape[1])))[:, :1]


def main_kernel(window, scale, fchunk,
                x_ref, dy_ref, kv_ref, cos_ref, sin_ref, pos_ref, kv_all,
                wq_ref, wo_ref, wg_ref, wu_ref, wd_ref, g_ai_ref, g_ao_ref, g_mi_ref, g_mo_ref, g_q_ref,
                y_ref, dmid_ref, q_ref, qp_ref, da_ref, lse_ref,
                big_out, kvp_all, dg_out,
                dwg, dwu, dwd, dwo, ga, gb, u_s, o_s, kvp_s, sems, load_sems, send_sems, recv_sems):
    step = pl.program_id(0)
    batch = kv_all.shape[0]
    me, ring = lax.axis_index("cp"), lax.axis_size("cp")
    right, left = lax.rem(me + 1, ring), lax.rem(me + ring - 1, ring)

    def halo(i):
        return pltpu.make_async_remote_copy(
            src_ref=kv_all.at[i], dst_ref=kvp_all.at[i], send_sem=send_sems.at[i], recv_sem=recv_sems.at[i],
            device_id={"cp": right}, device_id_type=MESH)

    def load(i):
        slot = lax.rem(i, 2)
        return pltpu.make_async_copy(kvp_all.at[i], kvp_s.at[slot], load_sems.at[slot])
    last = pl.num_programs(0) - 1
    tokens = x_ref.shape[1]
    head = g_q_ref.shape[1]
    heads = wq_ref.shape[1] // head
    chunks, qc = q_ref.shape[1], q_ref.shape[2] // heads
    keys = window + qc
    ffn = wg_ref.shape[1]

    @pl.when(step == 0)
    def _():
        barrier = pltpu.get_barrier_semaphore()
        for peer in (left, right):
            pl.semaphore_signal(barrier, inc=1, device_id={"cp": peer}, device_id_type=MESH)
        pl.semaphore_wait(barrier, 2)
        for i in range(batch):
            halo(i).start()
        for ref in (dwg, dwu, dwd, dwo, dg_out):
            ref[...] = jnp.zeros_like(ref)
        halo(0).wait_recv()
        load(0).start()

    load(step).wait()
    kvp_ref = kvp_s.at[pl.ds(lax.rem(step, 2), 1)]
    x = x_ref[0].astype(F32)
    n, _ = unit(x)
    h = (n * gain(g_ai_ref)).astype(BF16)
    g_q = gain(g_q_ref)
    pos_col = column_of(pos_ref[0])
    for c in range(chunks):
        rows = slice(c * qc, (c + 1) * qc)
        proj = dot(h[rows], wq_ref[...])
        cos, sin = cos_ref[0, rows], sin_ref[0, rows]
        bias = visible_bias(pos_ref, pos_col, c * qc, keys, qc, window, tokens)
        prev = kvp_ref[0, c * qc:]
        own = kv_ref[0, :(c + 1) * qc]
        k = jnp.concatenate([prev[:, :head], own[:, :head]], axis=0)
        v_t = jnp.transpose(jnp.concatenate([prev[:, head:], own[:, head:]], axis=0))
        for j in range(heads):
            raw = proj[:, j * head:(j + 1) * head]
            qp_ref[0, c, j * qc:(j + 1) * qc] = raw
            qn, _ = unit(raw)
            q = (rope(qn * g_q, cos, sin) * scale).astype(BF16)
            q_ref[0, c, j * qc:(j + 1) * qc] = q
            s = dot_nt(k, q) + bias
            top = jnp.max(s, axis=0, keepdims=True)
            e = jnp.exp(s - top)
            total = jnp.sum(e, axis=0, keepdims=True)
            p = (e * (1.0 / total)).astype(BF16)
            lse_ref[0, c, :, j * qc:(j + 1) * qc] = top + jnp.log(total)
            o_t = dot(v_t, p).astype(BF16)
            o_s[rows, j * head:(j + 1) * head] = jnp.transpose(o_t)

    @pl.when(step < last)
    def _():
        halo(step + 1).wait_recv()
        load(step + 1).start()

    o = o_s[...]
    o_proj = dot(o, wo_ref[...])
    on, o_r = unit(o_proj)
    m = (x + on * gain(g_ao_ref)).astype(BF16).astype(F32)
    mn, m_r = unit(m)
    b = (mn * gain(g_mi_ref)).astype(BF16)
    b_t = jnp.transpose(b)

    down = jnp.zeros_like(x)
    for f in range(ffn // fchunk):
        cols = slice(f * fchunk, (f + 1) * fchunk)
        gate = dot(b, wg_ref[:, cols])
        up = dot(b, wu_ref[:, cols])
        c0 = 0.7978845608028654
        g2 = gate * gate
        t = jnp.tanh(gate * (c0 + (c0 * 0.044715) * g2))
        half = 0.5 * t + 0.5
        act = gate * half
        slope = half + 0.5 * gate * (1.0 - t * t) * (c0 + (3.0 * c0 * 0.044715) * g2)
        ga[:, cols] = act
        gb[:, cols] = slope * up
        u = (act * up).astype(BF16)
        u_s[:, cols] = u
        down = down + dot(u, wd_ref[cols, :])
    dn, d_r = unit(down)
    dy = dy_ref[0].astype(F32)
    y_ref[0] = (m + dn * gain(g_mo_ref)).astype(BF16)
    dg_out[0:1] += colsum(dy * dn)
    d_down = unit_back(dn, d_r, dy * gain(g_mo_ref)).astype(BF16)
    d_down_t = jnp.transpose(d_down)
    d_b = jnp.zeros_like(x)
    for f in range(ffn // fchunk):
        cols = slice(f * fchunk, (f + 1) * fchunk)
        d_hid = dot_nt(d_down, wd_ref[cols, :]).astype(BF16).astype(F32)
        d_up = (d_hid * ga[:, cols]).astype(BF16)
        d_gate = (d_hid * gb[:, cols]).astype(BF16)
        dwd[:, cols] += dot(d_down_t, u_s[:, cols])
        dwg[:, cols] += dot(b_t, d_gate)
        dwu[:, cols] += dot(b_t, d_up)
        d_b = d_b + dot_nt(d_gate, wg_ref[:, cols]) + dot_nt(d_up, wu_ref[:, cols])
    dg_out[1:2] += colsum(d_b * mn)
    d_mid = dy + unit_back(mn, m_r, d_b * gain(g_mi_ref))
    dmid_ref[0] = d_mid
    dg_out[2:3] += colsum(d_mid * on)
    d_o = unit_back(on, o_r, d_mid * gain(g_ao_ref)).astype(BF16)
    dwo[...] += dot(jnp.transpose(d_o), o)
    d_attn = dot_nt(d_o, wo_ref[...]).astype(BF16)
    for c in range(chunks):
        for j in range(heads):
            da_ref[0, c, j * qc:(j + 1) * qc] = d_attn[c * qc:(c + 1) * qc, j * head:(j + 1) * head]

    @pl.when(step == last)
    def _():
        copies, at = [], 0
        for i, part in enumerate((dwg, dwu, dwd, dwo)):
            width = part.shape[1]
            copies.append(pltpu.make_async_copy(part, big_out.at[:, at:at + width], sems.at[i]))
            at += width
        for item in copies:
            item.start()
        for item in copies:
            item.wait()
        for i in range(batch):
            halo(i).wait_send()


def ring_steps(big_ref, core_buf, out_ref, own_v, send_v, recv_v, fin_v,
               core_send, core_recv, load_sem, rs_send, rs_recv, ag_send, ag_recv, p_send, p_recv, fin_sem):
    ring = lax.axis_size("cp")
    me = lax.axis_index("cp")
    n = ring // 2
    z, core = me // 2, lax.rem(me, 2)
    partner = z * 2 + 1 - core
    width = big_ref.shape[3] // 2
    cols = [slice(d * width, (d + 1) * width) for d in range(2)]
    nexts = [lax.rem(z + 1, n) * 2 + core, lax.rem(z + n - 1, n) * 2 + core]

    def rs_chunk(d, s):
        return lax.rem(z + n - s, n) if d == 0 else lax.rem(z + s, n)

    def ag_chunk(d, s):
        return lax.rem(z + 1 + n - s, n) if d == 0 else lax.rem(z + n - 1 + s, n)

    def remote(src, dst, send, recv, device):
        return pltpu.make_async_remote_copy(src_ref=src, dst_ref=dst, send_sem=send, recv_sem=recv,
                                            device_id={"cp": device}, device_id_type=MESH)

    def swap(d, s):
        c = rs_chunk(d, s)
        return remote(big_ref.at[1 - core, c, :, cols[d]], core_buf.at[c, :, cols[d]],
                      core_send.at[d, s], core_recv.at[d, s], partner)

    def loads(d, s):
        c, slot = rs_chunk(d, s), lax.rem(s, 2)
        return (pltpu.make_async_copy(big_ref.at[core, c, :, cols[d]], own_v.at[d, slot, 0], load_sem.at[d, slot, 0]),
                pltpu.make_async_copy(core_buf.at[c, :, cols[d]], own_v.at[d, slot, 1], load_sem.at[d, slot, 1]))

    def rs(d, s):
        return remote(send_v.at[d, lax.rem(s, 2)], recv_v.at[d, s], rs_send.at[d, s], rs_recv.at[d, s], nexts[d])

    def place(d, s):
        return out_ref.at[core, ag_chunk(d, s), :, cols[d]]

    def gather(d, s):
        return remote(place(d, s), place(d, s), ag_send.at[d, s], ag_recv.at[d, s], nexts[d])

    def share(d, s):
        return remote(place(d, s), place(d, s), p_send.at[d, s], p_recv.at[d, s], partner)

    def gather_first(d):
        return remote(fin_v.at[d], place(d, 0), ag_send.at[d, 0], ag_recv.at[d, 0], nexts[d])

    def share_first(d):
        return remote(fin_v.at[d], place(d, 0), p_send.at[d, 0], p_recv.at[d, 0], partner)

    def keep(d):
        return pltpu.make_async_copy(fin_v.at[d], place(d, 0), fin_sem.at[d])

    def start_loads(s):
        for d in range(2):
            swap(d, s).wait_recv()
            for item in loads(d, s):
                item.start()

    def step(u):
        @pl.when(u == 0)
        def _():
            @pl.loop(0, n)
            def _(s):
                for d in range(2):
                    swap(d, s).start()

        @pl.when(u == 1)
        def _():
            start_loads(0)

        s = u - 2

        @pl.when((s >= 0) & (s < n - 1))
        def _():
            for d in range(2):
                for item in loads(d, s):
                    item.wait()
            slot = lax.rem(s, 2)

            @pl.when(s >= 2)
            def _():
                for d in range(2):
                    rs(d, s - 2).wait_send()

            @pl.when(s == 0)
            def _():
                for d in range(2):
                    send_v[d, slot] = (own_v[d, slot, 0] + own_v[d, slot, 1]).astype(BF16)

            @pl.when(s > 0)
            def _():
                for d in range(2):
                    rs(d, s - 1).wait_recv()
                    send_v[d, slot] = (own_v[d, slot, 0] + own_v[d, slot, 1] + recv_v[d, s - 1].astype(F32)).astype(BF16)
            for d in range(2):
                rs(d, s).start()
            start_loads(s + 1)

        @pl.when(s == n - 1)
        def _():
            slot = (n - 1) % 2
            for d in range(2):
                for item in loads(d, n - 1):
                    item.wait()
                rs(d, n - 2).wait_recv()
                fin_v[d] = (own_v[d, slot, 0] + own_v[d, slot, 1] + recv_v[d, n - 2].astype(F32)).astype(BF16)
            for d in range(2):
                gather_first(d).start()
                share_first(d).start()
                keep(d).start()

        g = u - (n + 1)

        @pl.when((g >= 1) & (g < n))
        def _():
            for d in range(2):
                gather(d, g - 1).wait_recv()

            @pl.when(g < n - 1)
            def _():
                for d in range(2):
                    gather(d, g).start()
            for d in range(2):
                share(d, g).start()

        @pl.when(g == n - 1)
        def _():
            for d in range(2):
                keep(d).wait()
                for i in (n - 3, n - 2):
                    rs(d, i).wait_send()

            @pl.loop(0, n)
            def _(i):
                for d in range(2):
                    swap(d, i).wait_send()
                    share(d, i).wait_send()
                    share(d, i).wait_recv()

            @pl.loop(0, n - 1)
            def _(i):
                for d in range(2):
                    gather(d, i).wait_send()

    return step


def back_kernel(window, scale, batch,
                kv_ref, kvp_ref, cos_ref, sin_ref, pos_ref, q_ref, qp_ref, da_ref, lse_ref,
                x_ref, dmid_ref, cosp_ref, sinp_ref, big_ref,
                wqkv_ref, g_ai_ref, g_q_ref, g_k_ref,
                dx_ref, dw_ref, dgi_ref, dgq_ref, dgk_ref, full_ref, core_buf,
                p_s, s_s, ext, d_s, dkv_s, halo_out, halo_in, halo_send, halo_recv, *ring_refs):
    step = pl.program_id(0)
    tokens = x_ref.shape[1]
    head = g_q_ref.shape[1]
    chunks = q_ref.shape[1]
    q_dim = wqkv_ref.shape[1] - dkv_s.shape[2]
    heads = q_dim // head
    qc = q_ref.shape[2] // heads
    keys = window + qc
    me, ring = lax.axis_index("cp"), lax.axis_size("cp")
    left = lax.rem(me + ring - 1, ring)
    ring_step = ring_steps(big_ref, core_buf, full_ref, *ring_refs)

    def halo(i):
        slot = lax.rem(i, 2)
        return pltpu.make_async_remote_copy(
            src_ref=halo_out.at[slot], dst_ref=halo_in.at[i], send_sem=halo_send.at[slot], recv_sem=halo_recv.at[i],
            device_id={"cp": left}, device_id_type=MESH)

    @pl.when(step == 0)
    def _():
        barrier = pltpu.get_barrier_semaphore()
        for hop in (1, 2, ring - 1, ring - 2):
            pl.semaphore_signal(barrier, inc=1, device_id={"cp": lax.rem(me + hop, ring)}, device_id_type=MESH)
        pl.semaphore_wait(barrier, 4)
        for ref in (dw_ref, dgi_ref, dgq_ref, dgk_ref):
            ref[...] = jnp.zeros_like(ref)

    ring_step(2 * step)

    def attend(c):
        g_q = gain(g_q_ref)
        pos_col = column_of(pos_ref[0])
        rows = slice(c * qc, (c + 1) * qc)
        slot = lax.rem(step, 2)
        cos, sin = cos_ref[0, rows], sin_ref[0, rows]
        bias = visible_bias(pos_ref, pos_col, c * qc, keys, qc, window, tokens)
        prev = kvp_ref[0, c * qc:]
        own = kv_ref[0, :(c + 1) * qc]
        k = jnp.concatenate([prev[:, :head], own[:, :head]], axis=0)
        v = jnp.concatenate([prev[:, head:], own[:, head:]], axis=0)
        k_t = jnp.transpose(k)
        dg = jnp.zeros((1, head), F32)
        for j in range(heads):
            lanes = slice(j * qc, (j + 1) * qc)
            q = q_ref[0, c, lanes]
            d_o = da_ref[0, c, lanes]
            s = dot_nt(k, q) + bias
            p = jnp.exp(s - lse_ref[0, c, :, lanes])
            d_p = dot_nt(v, d_o)
            delta = jnp.sum(d_p * p, axis=0, keepdims=True)
            d_sc = (p * (d_p - delta)).astype(BF16)
            p_s[:, lanes] = p.astype(BF16)
            s_s[:, lanes] = d_sc
            d_q = jnp.transpose(dot(k_t, d_sc)) * scale
            qn, q_r = unit(qp_ref[0, c, lanes])
            d_qn = rope_back(d_q, cos, sin)
            dg = dg + colsum(d_qn * qn)
            d_s[slot, rows, j * head:(j + 1) * head] = unit_back(qn, q_r, d_qn * g_q).astype(BF16)
        dgq_ref[...] += dg
        span = slice(c * qc, c * qc + keys)
        d_k = dot(s_s[...], q_ref[0, c])
        d_v = dot(p_s[...], da_ref[0, c])
        if c == 0:
            ext[span, :head] = d_k
            ext[span, head:] = d_v
            ext[keys:] = jnp.zeros_like(ext[keys:])
        else:
            ext[span, :head] += d_k
            ext[span, head:] += d_v

    @pl.when(step < batch)
    def _():
        attend(0)

    ring_step(2 * step + 1)

    @pl.when(step < batch)
    def _():
        for c in range(1, chunks):
            attend(c)
        slot = lax.rem(step, 2)

        @pl.when(step >= 2)
        def _():
            halo(step - 2).wait_send()
        halo_out[slot] = ext[:window].astype(BF16)
        dkv_s[slot] = ext[window:]
        halo(step).start()

    @pl.when(step > 0)
    def _():
        slot = lax.rem(step + 1, 2)
        n, r = unit(x_ref[0].astype(F32))
        g_ai = gain(g_ai_ref)
        h = (n * g_ai).astype(BF16)
        kn, k_r = unit(dot(h, wqkv_ref[:, q_dim:q_dim + head]))
        halo(step - 1).wait_recv()
        total = dkv_s[slot] + halo_in[step - 1].astype(F32)
        d_kn = rope_back(total[:, :head], cosp_ref[0], sinp_ref[0])
        dgk_ref[...] += colsum(d_kn * kn)
        d_s[slot, :, q_dim:q_dim + head] = unit_back(kn, k_r, d_kn * gain(g_k_ref)).astype(BF16)
        d_s[slot, :, q_dim + head:] = total[:, head:].astype(BF16)
        d_all = d_s[slot]
        dw_ref[...] += dot(jnp.transpose(h), d_all)
        d_h = dot_nt(d_all, wqkv_ref[...])
        dgi_ref[...] += colsum(d_h * n)
        dx_ref[0] = (dmid_ref[0] + unit_back(n, r, d_h * g_ai)).astype(BF16)

    @pl.when(step == batch)
    def _():
        halo(batch - 2).wait_send()
        halo(batch - 1).wait_send()


def per_seq(shape, lag=None, **kw):
    tail = tuple(shape[1:])
    top = shape[0] - 1
    if lag is None:
        return pl.BlockSpec((1,) + tail, lambda b: (b,) + (0,) * len(tail), **kw)
    return pl.BlockSpec((1,) + tail, lambda b: (jnp.clip(b - lag, 0, top),) + (0,) * len(tail), **kw)


def whole(shape):
    return pl.BlockSpec(tuple(shape), lambda b: (0,) * len(shape), pipeline_mode=pl.Buffered(1))


ANY = pl.BlockSpec(memory_space=pl.ANY)


def call(kernel, steps, ins, in_specs, outs, out_specs, scratch, flops, **params):
    nbytes = sum(a.size * a.dtype.itemsize for a in ins) + sum(o.size * o.dtype.itemsize for o in outs)
    return pl.pallas_call(
        kernel, grid=(steps,), in_specs=in_specs, out_specs=out_specs, out_shape=outs, scratch_shapes=scratch,
        compiler_params=pltpu.CompilerParams(dimension_semantics=("arbitrary",), vmem_limit_bytes=VMEM_CAP, **params),
        cost_estimate=pl.CostEstimate(flops=flops, bytes_accessed=nbytes, transcendentals=0),
    )(*ins)


def solution(mesh):
    cp_size = mesh.shape["cp"]
    to_next = [(idx, idx + 1) for idx in range(cp_size - 1)]

    def local_step(x, dy, positions, w_query, w_key, w_value, w_out, w_gate, w_up, w_down, g_attn_in, g_attn_out, g_mlp_in, g_mlp_out, g_query, g_key):
        n_batch, tokens, dim = x.shape
        head = g_query.shape[0]
        q_dim = w_query.shape[1]
        kv_dim = w_key.shape[1] + w_value.shape[1]
        heads = q_dim // head
        ffn = w_gate.shape[1]
        window = window_size(dim)
        scale = score_scale(dim, heads, head)
        qc = min(256, tokens)
        chunks = tokens // qc
        keys = window + qc
        shard_idx = lax.axis_index("cp")
        sds = jax.ShapeDtypeStruct
        n_tok = n_batch * tokens
        chips = cp_size // 2
        wide = 3 * ffn + q_dim
        slab = dim // cp_size
        dma = pltpu.SemaphoreType.DMA

        half = head // 2
        inv_freq = ROPE_BASE ** (-2.0 * jnp.arange(half, dtype=F32) / head)
        angles = positions.astype(F32)[..., None] * inv_freq
        cos, sin = jnp.cos(angles), jnp.sin(angles)
        row = lambda g: g.reshape(1, -1)
        w_kv = jnp.concatenate([w_key, w_value], axis=1)
        w_qkv = jnp.concatenate([w_query, w_kv], axis=1)
        g_ai, g_ao, g_mi, g_mo, g_q, g_k = map(row, (g_attn_in, g_attn_out, g_mlp_in, g_mlp_out, g_query, g_key))
        pos_prev = lax.ppermute(positions, "cp", to_next)
        pos_prev = jnp.where(shard_idx > 0, pos_prev, -(2 ** 30))
        pos_ext = jnp.concatenate([pos_prev, positions], axis=1)[:, None, :]
        cs = per_seq(cos.shape)

        (kv,) = call(kv_kernel, n_batch, [x, cos, sin, w_kv, g_ai, g_k],
                     [per_seq(x.shape), cs, cs, whole(w_kv.shape), whole(g_ai.shape), whole(g_k.shape)],
                     [sds((n_batch, tokens, kv_dim), BF16)], [per_seq((n_batch, tokens, kv_dim))], [], 2 * n_tok * dim * kv_dim)

        stack = (n_batch, chunks, heads * qc, head)
        weights = [w_query, w_out, w_gate, w_up, w_down, g_ai, g_ao, g_mi, g_mo, g_q]
        lse_shape = (n_batch, chunks, 1, heads * qc)
        xs = per_seq(x.shape)
        y, d_mid, q_st, qp_st, da_st, lse, big, kv_prev, dg_main = call(
            functools.partial(main_kernel, window, scale, 512), n_batch,
            [x, dy, kv, cos, sin, pos_ext, kv] + weights,
            [xs, xs, per_seq(kv.shape), cs, cs, per_seq(pos_ext.shape), ANY] + [whole(w.shape) for w in weights],
            [sds(x.shape, BF16), sds(x.shape, F32), sds(stack, BF16), sds(stack, F32), sds(stack, BF16), sds(lse_shape, F32),
             sds((dim, wide), F32), sds(kv.shape, BF16), sds((8, dim), F32)],
            [xs, xs, per_seq(stack), per_seq(stack, pipeline_mode=pl.Buffered(1)), per_seq(stack), per_seq(lse_shape),
             ANY, ANY, whole((8, dim))],
            [pltpu.VMEM((dim, ffn), F32)] * 3 + [pltpu.VMEM((dim, q_dim), F32)]
            + [pltpu.VMEM((tokens, ffn), F32)] * 2 + [pltpu.VMEM((tokens, ffn), BF16), pltpu.VMEM((tokens, q_dim), BF16),
                                                     pltpu.VMEM((2, tokens, kv_dim), BF16),
                                                     dma((4,)), dma((2,)), dma((n_batch,)), dma((n_batch,))],
            2 * n_tok * (9 * dim * ffn + 4 * dim * q_dim + 2 * q_dim * keys),
            collective_id=0, has_side_effects=True)

        big = big.reshape(2, chips, slab, wide)
        part = (slab, wide // 2)
        first, behind = (lambda a: per_seq(a.shape, 0)), (lambda a: per_seq(a.shape, 1))
        seq_in = [kv, kv_prev, cos, sin, pos_ext, q_st, qp_st, da_st, lse]
        lag_in = [x, d_mid, cos, sin]
        back_w = [w_qkv, g_ai, g_q, g_k]
        dx, dw, dgi, dgq, dgk, full, _ = call(
            functools.partial(back_kernel, window, scale, n_batch), n_batch + 1,
            seq_in + lag_in + [big] + back_w,
            [first(a) for a in seq_in] + [behind(a) for a in lag_in] + [ANY] + [whole(w.shape) for w in back_w],
            [sds(x.shape, BF16), sds(w_qkv.shape, F32), sds((1, dim), F32), sds((1, head), F32), sds((1, head), F32),
             sds(big.shape, BF16), sds(big.shape[1:], F32)],
            [behind(x), whole(w_qkv.shape), whole((1, dim)), whole((1, head)), whole((1, head)), ANY, ANY],
            [pltpu.VMEM((keys, heads * qc), BF16)] * 2
            + [pltpu.VMEM((window + tokens, kv_dim), F32), pltpu.VMEM((2, tokens, q_dim + kv_dim), BF16),
               pltpu.VMEM((2, tokens, kv_dim), F32), pltpu.VMEM((2, window, kv_dim), BF16),
               pltpu.VMEM((n_batch, window, kv_dim), BF16), dma((2,)), dma((n_batch,)),
               pltpu.VMEM((2, 2, 2) + part, F32), pltpu.VMEM((2, 2) + part, BF16),
               pltpu.VMEM((2, chips - 1) + part, BF16), pltpu.VMEM((2,) + part, BF16),
               dma((2, chips)), dma((2, chips)), dma((2, 2, 2)), dma((2, chips - 1)), dma((2, chips - 1)),
               dma((2, chips - 1)), dma((2, chips - 1)), dma((2, chips)), dma((2, chips)), dma((2,))],
            2 * n_tok * (2 * dim * (q_dim + kv_dim) + 5 * q_dim * keys),
            collective_id=1, has_side_effects=True)

        full = full.reshape(dim, wide)
        r_dw, r_dg, r_dgq, r_dgi, r_dgk = lax.psum((dw, dg_main, dgq, dgi, dgk), "cp")
        b16 = lambda v: v.astype(BF16)
        kv_half = q_dim + kv_dim // 2
        return (y, dx, b16(r_dw[:, :q_dim]), b16(r_dw[:, q_dim:kv_half]), b16(r_dw[:, kv_half:]), full[:, 3 * ffn:].T,
                full[:, :ffn], full[:, ffn:2 * ffn], full[:, 2 * ffn:3 * ffn].T,
                b16(r_dgi[0]), b16(r_dg[2]), b16(r_dg[1]), b16(r_dg[0]), b16(r_dgq[0]), b16(r_dgk[0]))

    seq_spec = P("dp", "cp", None)
    in_specs = (seq_spec, seq_spec, P("dp", "cp")) + (P(None, None),) * 7 + (P(None),) * 6
    out_specs = (seq_spec, seq_spec) + (P("dp", None),) * 7 + (P("dp"),) * 6
    return jax.shard_map(local_step, mesh=mesh, in_specs=in_specs, out_specs=out_specs, check_vma=False)
```

```python
import functools
import jax
import jax.numpy as jnp
from jax import lax
from jax.experimental import pallas as pl
from jax.experimental.pallas import tpu as pltpu
from jax.sharding import PartitionSpec as P

NORM_EPS = 1e-6
ROPE_BASE = 10000.0
NEG = -1e30
F32 = jnp.float32
BF16 = jnp.bfloat16
VMEM_CAP = 67000000
MESH = pl.DeviceIdType.MESH


def window_size(model_dim):
    return 512 * min(2, 1 + model_dim // 2048)


def score_scale(model_dim, num_heads, head_dim):
    scalar = 256 if head_dim == 256 else model_dim // num_heads
    return scalar ** -0.5


def dot(a, b):
    return jnp.dot(a, b, preferred_element_type=F32)


def dot_nt(a, b):
    return lax.dot_general(a, b, (((1,), (1,)), ((), ())), preferred_element_type=F32)


def unit(v):
    r = lax.rsqrt(jnp.mean(v * v, axis=-1, keepdims=True) + NORM_EPS)
    return v * r, r


def unit_back(n, r, t):
    return r * (t - n * jnp.mean(t * n, axis=-1, keepdims=True))


def rope(n, cos, sin):
    half = n.shape[-1] // 2
    a, b = n[:, :half], n[:, half:]
    return jnp.concatenate([a * cos - b * sin, b * cos + a * sin], axis=-1)


def rope_back(d, cos, sin):
    half = d.shape[-1] // 2
    a, b = d[:, :half], d[:, half:]
    return jnp.concatenate([a * cos + b * sin, b * cos - a * sin], axis=-1)


def gains(ref, dim, head, *rows):
    return [ref.at[i:i + 1, :dim if i < 4 else head] for i in rows]


def gain(ref):
    return 1.0 + ref[...]


def colsum(v):
    return jnp.sum(v, axis=0, keepdims=True)


def kv_kernel(x_ref, cos_ref, sin_ref, wk_ref, wv_ref, g_ref, kv_ref):
    head = wk_ref.shape[1]
    g_in_ref, g_k_ref = gains(g_ref, x_ref.shape[2], head, 0, 5)
    n, _ = unit(x_ref[0].astype(F32))
    h = (n * gain(g_in_ref)).astype(BF16)
    kn, _ = unit(dot(h, wk_ref[...]))
    k = rope(kn * gain(g_k_ref), cos_ref[0], sin_ref[0])
    kv_ref[0, :, :head] = k.astype(BF16)
    kv_ref[0, :, head:] = dot(h, wv_ref[...]).astype(BF16)


def visible_bias(pos_ref, pos_col, first, keys, queries, window, tokens):
    key_pos = pos_col[first:first + keys]
    query_pos = pos_ref[0, :, tokens + first:tokens + first + queries]
    seen = (key_pos > query_pos - window) & (key_pos <= query_pos)
    return jnp.where(seen, 0.0, NEG).astype(F32)


def column_of(row):
    return jnp.transpose(jnp.broadcast_to(row, (8, row.shape[1])))[:, :1]


def main_kernel(window, scale, fchunk,
                x_ref, dy_ref, kv_ref, cos_ref, sin_ref, pos_ref, kv_all,
                wq_ref, wo_ref, wg_ref, wu_ref, wd_ref, g_ref,
                y_ref, dmid_ref, q_ref, qp_ref, da_ref, lse_ref,
                big_out, kvp_all, dg_out,
                dwg, dwu, dwd, dwo, ga, gb, u_s, o_s, kvp_s, sems, load_sems, send_sems, recv_sems):
    step = pl.program_id(0)
    batch = kv_all.shape[0]
    me, ring = lax.axis_index("cp"), lax.axis_size("cp")
    right, left = lax.rem(me + 1, ring), lax.rem(me + ring - 1, ring)

    def halo(i):
        return pltpu.make_async_remote_copy(
            src_ref=kv_all.at[i], dst_ref=kvp_all.at[i], send_sem=send_sems.at[i], recv_sem=recv_sems.at[i],
            device_id={"cp": right}, device_id_type=MESH)

    def load(i):
        slot = lax.rem(i, 2)
        return pltpu.make_async_copy(kvp_all.at[i], kvp_s.at[slot], load_sems.at[slot])
    last = pl.num_programs(0) - 1
    tokens = x_ref.shape[1]
    head = q_ref.shape[3]
    g_ai_ref, g_ao_ref, g_mi_ref, g_mo_ref, g_q_ref = gains(g_ref, x_ref.shape[2], head, 0, 1, 2, 3, 4)
    heads = wq_ref.shape[1] // head
    chunks, qc = q_ref.shape[1], q_ref.shape[2] // heads
    keys = window + qc
    ffn = wg_ref.shape[1]

    @pl.when(step == 0)
    def _():
        barrier = pltpu.get_barrier_semaphore()
        for peer in (left, right):
            pl.semaphore_signal(barrier, inc=1, device_id={"cp": peer}, device_id_type=MESH)
        pl.semaphore_wait(barrier, 2)
        for i in range(batch):
            halo(i).start()
        for ref in (dwg, dwu, dwd, dwo, dg_out):
            ref[...] = jnp.zeros_like(ref)
        halo(0).wait_recv()
        load(0).start()

    load(step).wait()
    kvp_ref = kvp_s.at[pl.ds(lax.rem(step, 2), 1)]
    x = x_ref[0].astype(F32)
    n, _ = unit(x)
    h = (n * gain(g_ai_ref)).astype(BF16)
    g_q = gain(g_q_ref)
    pos_col = column_of(pos_ref[0])
    for c in range(chunks):
        rows = slice(c * qc, (c + 1) * qc)
        proj = dot(h[rows], wq_ref[...])
        cos, sin = cos_ref[0, rows], sin_ref[0, rows]
        bias = visible_bias(pos_ref, pos_col, c * qc, keys, qc, window, tokens)
        prev = kvp_ref[0, c * qc:]
        own = kv_ref[0, :(c + 1) * qc]
        k = jnp.concatenate([prev[:, :head], own[:, :head]], axis=0)
        v_t = jnp.transpose(jnp.concatenate([prev[:, head:], own[:, head:]], axis=0))
        for j in range(heads):
            raw = proj[:, j * head:(j + 1) * head]
            qp_ref[0, c, j * qc:(j + 1) * qc] = raw
            qn, _ = unit(raw)
            q = (rope(qn * g_q, cos, sin) * scale).astype(BF16)
            q_ref[0, c, j * qc:(j + 1) * qc] = q
            s = dot_nt(k, q) + bias
            top = jnp.max(s, axis=0, keepdims=True)
            e = jnp.exp(s - top)
            total = jnp.sum(e, axis=0, keepdims=True)
            p = (e * (1.0 / total)).astype(BF16)
            lse_ref[0, c, :, j * qc:(j + 1) * qc] = top + jnp.log(total)
            o_t = dot(v_t, p).astype(BF16)
            o_s[rows, j * head:(j + 1) * head] = jnp.transpose(o_t)

    @pl.when(step < last)
    def _():
        halo(step + 1).wait_recv()
        load(step + 1).start()

    o = o_s[...]
    o_proj = dot(o, wo_ref[...])
    on, o_r = unit(o_proj)
    m = (x + on * gain(g_ao_ref)).astype(BF16).astype(F32)
    mn, m_r = unit(m)
    b = (mn * gain(g_mi_ref)).astype(BF16)
    b_t = jnp.transpose(b)

    acc = dmid_ref.at[0]
    acc[...] = jnp.zeros_like(x)

    @pl.loop(0, ffn // fchunk)
    def _(f):
        cols = pl.ds(pl.multiple_of(f * fchunk, fchunk), fchunk)
        gate = dot(b, wg_ref[:, cols])
        up = dot(b, wu_ref[:, cols])
        c0 = 0.7978845608028654
        g2 = gate * gate
        t = jnp.tanh(gate * (c0 + (c0 * 0.044715) * g2))
        half = 0.5 * t + 0.5
        act = gate * half
        slope = half + 0.5 * gate * (1.0 - t * t) * (c0 + (3.0 * c0 * 0.044715) * g2)
        ga[:, cols] = act
        gb[:, cols] = slope * up
        u = (act * up).astype(BF16)
        u_s[:, cols] = u
        acc[...] += dot(u, wd_ref[cols, :])

    down = acc[...]
    dn, d_r = unit(down)
    dy = dy_ref[0].astype(F32)
    y_ref[0] = (m + dn * gain(g_mo_ref)).astype(BF16)
    dg_out[0:1] += colsum(dy * dn)
    d_down = unit_back(dn, d_r, dy * gain(g_mo_ref)).astype(BF16)
    d_down_t = jnp.transpose(d_down)
    acc[...] = jnp.zeros_like(x)

    @pl.loop(0, ffn // fchunk)
    def _(f):
        cols = pl.ds(pl.multiple_of(f * fchunk, fchunk), fchunk)
        d_hid = dot_nt(d_down, wd_ref[cols, :]).astype(BF16).astype(F32)
        d_up = (d_hid * ga[:, cols]).astype(BF16)
        d_gate = (d_hid * gb[:, cols]).astype(BF16)
        dwd[:, cols] += dot(d_down_t, u_s[:, cols])
        dwg[:, cols] += dot(b_t, d_gate)
        dwu[:, cols] += dot(b_t, d_up)
        acc[...] += dot_nt(d_gate, wg_ref[:, cols]) + dot_nt(d_up, wu_ref[:, cols])

    d_b = acc[...]
    dg_out[1:2] += colsum(d_b * mn)
    d_mid = dy + unit_back(mn, m_r, d_b * gain(g_mi_ref))
    dmid_ref[0] = d_mid
    dg_out[2:3] += colsum(d_mid * on)
    d_o = unit_back(on, o_r, d_mid * gain(g_ao_ref)).astype(BF16)
    dwo[...] += dot(jnp.transpose(d_o), o)
    d_attn = dot_nt(d_o, wo_ref[...]).astype(BF16)
    for c in range(chunks):
        for j in range(heads):
            da_ref[0, c, j * qc:(j + 1) * qc] = d_attn[c * qc:(c + 1) * qc, j * head:(j + 1) * head]

    @pl.when(step == last)
    def _():
        copies, at = [], 0
        for i, part in enumerate((dwg, dwu, dwd, dwo)):
            width = part.shape[1]
            copies.append(pltpu.make_async_copy(part, big_out.at[:, at:at + width], sems.at[i]))
            at += width
        for item in copies:
            item.start()
        for item in copies:
            item.wait()
        for i in range(batch):
            halo(i).wait_send()


def ring_steps(cols, big_ref, core_buf, out_ref, own_v, send_v, recv_v, fin_v,
               core_send, core_recv, load_sem, rs_send, rs_recv, ag_send, ag_recv, p_send, p_recv, fin_sem):
    ring = lax.axis_size("cp")
    me = lax.axis_index("cp")
    n = ring // 2
    z, core = me // 2, lax.rem(me, 2)
    partner = z * 2 + 1 - core
    part = [slice(0, c.stop - c.start) for c in cols]
    nexts = [lax.rem(z + 1, n) * 2 + core, lax.rem(z + n - 1, n) * 2 + core]

    def rs_chunk(d, s):
        return lax.rem(z + n - s, n) if d == 0 else lax.rem(z + s, n)

    def ag_chunk(d, s):
        return lax.rem(z + 1 + n - s, n) if d == 0 else lax.rem(z + n - 1 + s, n)

    def remote(src, dst, send, recv, device):
        return pltpu.make_async_remote_copy(src_ref=src, dst_ref=dst, send_sem=send, recv_sem=recv,
                                            device_id={"cp": device}, device_id_type=MESH)

    def swap(d, s):
        c = rs_chunk(d, s)
        return remote(big_ref.at[1 - core, c, :, cols[d]], core_buf.at[c, :, cols[d]],
                      core_send.at[d, s], core_recv.at[d, s], partner)

    def loads(d, s):
        c, slot = rs_chunk(d, s), lax.rem(s, 2)
        return (pltpu.make_async_copy(big_ref.at[core, c, :, cols[d]], own_v.at[d, slot, 0, :, part[d]], load_sem.at[d, slot, 0]),
                pltpu.make_async_copy(core_buf.at[c, :, cols[d]], own_v.at[d, slot, 1, :, part[d]], load_sem.at[d, slot, 1]))

    def rs(d, s):
        return remote(send_v.at[d, lax.rem(s, 2), :, part[d]], recv_v.at[d, s, :, part[d]], rs_send.at[d, s], rs_recv.at[d, s], nexts[d])

    def place(d, s):
        return out_ref.at[core, ag_chunk(d, s), :, cols[d]]

    def gather(d, s):
        return remote(place(d, s), place(d, s), ag_send.at[d, s], ag_recv.at[d, s], nexts[d])

    def share(d, s):
        return remote(place(d, s), place(d, s), p_send.at[d, s], p_recv.at[d, s], partner)

    def gather_first(d):
        return remote(fin_v.at[d, :, part[d]], place(d, 0), ag_send.at[d, 0], ag_recv.at[d, 0], nexts[d])

    def share_first(d):
        return remote(fin_v.at[d, :, part[d]], place(d, 0), p_send.at[d, 0], p_recv.at[d, 0], partner)

    def keep(d):
        return pltpu.make_async_copy(fin_v.at[d, :, part[d]], place(d, 0), fin_sem.at[d])

    def start_loads(s):
        for d in range(2):
            swap(d, s).wait_recv()
            for item in loads(d, s):
                item.start()

    def step(u):
        @pl.when(u == 0)
        def _():
            @pl.loop(0, n)
            def _(s):
                for d in range(2):
                    swap(d, s).start()

        @pl.when(u == 1)
        def _():
            start_loads(0)

        s = u - 2

        @pl.when((s >= 0) & (s < n - 1))
        def _():
            for d in range(2):
                for item in loads(d, s):
                    item.wait()
            slot = lax.rem(s, 2)

            @pl.when(s >= 2)
            def _():
                for d in range(2):
                    rs(d, s - 2).wait_send()

            @pl.when(s == 0)
            def _():
                for d in range(2):
                    w = part[d]
                    send_v[d, slot, :, w] = (own_v[d, slot, 0, :, w] + own_v[d, slot, 1, :, w]).astype(BF16)

            @pl.when(s > 0)
            def _():
                for d in range(2):
                    rs(d, s - 1).wait_recv()
                    w = part[d]
                    send_v[d, slot, :, w] = (own_v[d, slot, 0, :, w] + own_v[d, slot, 1, :, w]
                                             + recv_v[d, s - 1, :, w].astype(F32)).astype(BF16)
            for d in range(2):
                rs(d, s).start()
            start_loads(s + 1)

        @pl.when(s == n - 1)
        def _():
            slot = (n - 1) % 2
            for d in range(2):
                for item in loads(d, n - 1):
                    item.wait()
                rs(d, n - 2).wait_recv()
                w = part[d]
                fin_v[d, :, w] = (own_v[d, slot, 0, :, w] + own_v[d, slot, 1, :, w]
                                  + recv_v[d, n - 2, :, w].astype(F32)).astype(BF16)
            for d in range(2):
                gather_first(d).start()
                share_first(d).start()
                keep(d).start()

        g = u - (n + 1)

        @pl.when((g >= 1) & (g < n))
        def _():
            for d in range(2):
                gather(d, g - 1).wait_recv()

            @pl.when(g < n - 1)
            def _():
                for d in range(2):
                    gather(d, g).start()
            for d in range(2):
                share(d, g).start()

        @pl.when(g == n - 1)
        def _():
            for d in range(2):
                keep(d).wait()
                for i in (n - 3, n - 2):
                    rs(d, i).wait_send()

            @pl.loop(0, n)
            def _(i):
                for d in range(2):
                    swap(d, i).wait_send()
                    share(d, i).wait_send()
                    share(d, i).wait_recv()

            @pl.loop(0, n - 1)
            def _(i):
                for d in range(2):
                    gather(d, i).wait_send()

    return step


def piece_widths(wide):
    tiles = wide // 128
    down = tiles * 5 // 28
    return (tiles // 2 - down) * 128, down * 128


def back_kernel(window, scale, batch,
                kv_ref, kvp_ref, cos_ref, sin_ref, pos_ref, q_ref, qp_ref, da_ref, lse_ref,
                x_ref, dmid_ref, cosp_ref, sinp_ref, big_ref,
                wq_ref, wk_ref, wv_ref, g_ref,
                dx_ref, dw_ref, dgi_ref, dgq_ref, dgk_ref, full_ref, core_buf,
                p_s, s_s, ext, d_s, dkv_s, halo_out, halo_in, halo_send, halo_recv, *ring_refs):
    step = pl.program_id(0)
    tokens = x_ref.shape[1]
    head = q_ref.shape[3]
    g_ai_ref, g_q_ref, g_k_ref = gains(g_ref, x_ref.shape[2], head, 0, 4, 5)
    chunks = q_ref.shape[1]
    q_dim = wq_ref.shape[1]
    heads = q_dim // head
    qc = q_ref.shape[2] // heads
    keys = window + qc
    me, ring = lax.axis_index("cp"), lax.axis_size("cp")
    left = lax.rem(me + ring - 1, ring)
    per_ring = len(ring_refs) // 2
    up_w, down_w = piece_widths(big_ref.shape[3])
    ring_a, ring_b = [
        ring_steps([slice(i * up_w, (i + 1) * up_w), slice(2 * up_w + i * down_w, 2 * up_w + (i + 1) * down_w)],
                   big_ref, core_buf, full_ref, *ring_refs[i * per_ring:(i + 1) * per_ring])
        for i in range(2)]

    def halo(i, part):
        slot = lax.rem(i, 2)
        cols = slice(part * head, (part + 1) * head)
        return pltpu.make_async_remote_copy(
            src_ref=halo_out.at[slot, :, cols], dst_ref=halo_in.at[i, :, cols],
            send_sem=halo_send.at[slot, part], recv_sem=halo_recv.at[i, part],
            device_id={"cp": left}, device_id_type=MESH)

    @pl.when(step == 0)
    def _():
        barrier = pltpu.get_barrier_semaphore()
        for hop in (1, 2, ring - 1, ring - 2):
            pl.semaphore_signal(barrier, inc=1, device_id={"cp": lax.rem(me + hop, ring)}, device_id_type=MESH)
        pl.semaphore_wait(barrier, 4)
        for ref in (dw_ref, dgi_ref, dgq_ref, dgk_ref):
            ref[...] = jnp.zeros_like(ref)

    ring_a(2 * step)
    ring_b(2 * step)

    def attend(c):
        g_q = gain(g_q_ref)
        pos_col = column_of(pos_ref[0])
        rows = slice(c * qc, (c + 1) * qc)
        slot = lax.rem(step, 2)
        cos, sin = cos_ref[0, rows], sin_ref[0, rows]
        bias = visible_bias(pos_ref, pos_col, c * qc, keys, qc, window, tokens)
        prev = kvp_ref[0, c * qc:]
        own = kv_ref[0, :(c + 1) * qc]
        k = jnp.concatenate([prev[:, :head], own[:, :head]], axis=0)
        v = jnp.concatenate([prev[:, head:], own[:, head:]], axis=0)
        k_t = jnp.transpose(k)
        dg = jnp.zeros((1, head), F32)
        for j in range(heads):
            lanes = slice(j * qc, (j + 1) * qc)
            q = q_ref[0, c, lanes]
            d_o = da_ref[0, c, lanes]
            s = dot_nt(k, q) + bias
            p = jnp.exp(s - lse_ref[0, c, :, lanes])
            d_p = dot_nt(v, d_o)
            delta = jnp.sum(d_p * p, axis=0, keepdims=True)
            d_sc = (p * (d_p - delta)).astype(BF16)
            p_s[:, lanes] = p.astype(BF16)
            s_s[:, lanes] = d_sc
            d_q = jnp.transpose(dot(k_t, d_sc)) * scale
            qn, q_r = unit(qp_ref[0, c, lanes])
            d_qn = rope_back(d_q, cos, sin)
            dg = dg + colsum(d_qn * qn)
            d_s[slot, rows, j * head:(j + 1) * head] = unit_back(qn, q_r, d_qn * g_q).astype(BF16)
        dgq_ref[...] += dg
        span = slice(c * qc, c * qc + keys)
        d_k = dot(s_s[...], q_ref[0, c])
        d_v = dot(p_s[...], da_ref[0, c])
        if c == 0:
            ext[span, :head] = d_k
            ext[span, head:] = d_v
            ext[keys:] = jnp.zeros_like(ext[keys:])
        else:
            ext[span, :head] += d_k
            ext[span, head:] += d_v

    @pl.when(step < batch)
    def _():
        attend(0)

    ring_a(2 * step + 1)
    ring_b(2 * step + 1)

    @pl.when(step > 0)
    def _():
        halo(step - 1, 1).start()

    @pl.when(step < batch)
    def _():
        for c in range(1, chunks):
            attend(c)
        slot = lax.rem(step, 2)

        @pl.when(step >= 2)
        def _():
            for part in range(2):
                halo(step - 2, part).wait_send()
        halo_out[slot] = ext[:window].astype(BF16)
        dkv_s[slot] = ext[window:]
        halo(step, 0).start()

    @pl.when(step > 0)
    def _():
        slot = lax.rem(step + 1, 2)
        n, r = unit(x_ref[0].astype(F32))
        g_ai = gain(g_ai_ref)
        h = (n * g_ai).astype(BF16)
        kn, k_r = unit(dot(h, wk_ref[...]))
        for part in range(2):
            halo(step - 1, part).wait_recv()
        total = dkv_s[slot] + halo_in[step - 1].astype(F32)
        d_kn = rope_back(total[:, :head], cosp_ref[0], sinp_ref[0])
        dgk_ref[...] += colsum(d_kn * kn)
        d_s[slot, :, q_dim:q_dim + head] = unit_back(kn, k_r, d_kn * gain(g_k_ref)).astype(BF16)
        d_s[slot, :, q_dim + head:] = total[:, head:].astype(BF16)
        d_all = d_s[slot]
        dw_ref[...] += dot(jnp.transpose(h), d_all)
        d_h = (dot_nt(d_all[:, :q_dim], wq_ref[...]) + dot_nt(d_all[:, q_dim:q_dim + head], wk_ref[...])
               + dot_nt(d_all[:, q_dim + head:], wv_ref[...]))
        dgi_ref[...] += colsum(d_h * n)
        dx_ref[0] = (dmid_ref[0] + unit_back(n, r, d_h * g_ai)).astype(BF16)

    @pl.when(step == batch)
    def _():
        for i in (batch - 2, batch - 1):
            for part in range(2):
                halo(i, part).wait_send()


def per_seq(shape, lag=None, **kw):
    tail = tuple(shape[1:])
    top = shape[0] - 1
    if lag is None:
        return pl.BlockSpec((1,) + tail, lambda b: (b,) + (0,) * len(tail), **kw)
    return pl.BlockSpec((1,) + tail, lambda b: (jnp.clip(b - lag, 0, top),) + (0,) * len(tail), **kw)


def whole(shape):
    return pl.BlockSpec(tuple(shape), lambda b: (0,) * len(shape), pipeline_mode=pl.Buffered(1))


ANY = pl.BlockSpec(memory_space=pl.ANY)


def call(kernel, steps, ins, in_specs, outs, out_specs, scratch, flops, **params):
    nbytes = sum(a.size * a.dtype.itemsize for a in ins) + sum(o.size * o.dtype.itemsize for o in outs)
    return pl.pallas_call(
        kernel, grid=(steps,), in_specs=in_specs, out_specs=out_specs, out_shape=outs, scratch_shapes=scratch,
        compiler_params=pltpu.CompilerParams(dimension_semantics=("arbitrary",), vmem_limit_bytes=VMEM_CAP, **params),
        cost_estimate=pl.CostEstimate(flops=flops, bytes_accessed=nbytes, transcendentals=0),
    )(*ins)


def solution(mesh):
    cp_size = mesh.shape["cp"]
    to_next = [(idx, idx + 1) for idx in range(cp_size - 1)]

    def local_step(x, dy, positions, w_query, w_key, w_value, w_out, w_gate, w_up, w_down, g_attn_in, g_attn_out, g_mlp_in, g_mlp_out, g_query, g_key):
        n_batch, tokens, dim = x.shape
        head = g_query.shape[0]
        q_dim = w_query.shape[1]
        kv_dim = w_key.shape[1] + w_value.shape[1]
        heads = q_dim // head
        ffn = w_gate.shape[1]
        window = window_size(dim)
        scale = score_scale(dim, heads, head)
        qc = min(256, tokens)
        chunks = tokens // qc
        keys = window + qc
        shard_idx = lax.axis_index("cp")
        sds = jax.ShapeDtypeStruct
        n_tok = n_batch * tokens
        chips = cp_size // 2
        wide = 3 * ffn + q_dim
        slab = dim // cp_size
        dma = pltpu.SemaphoreType.DMA

        half = head // 2
        inv_freq = ROPE_BASE ** (-2.0 * jnp.arange(half, dtype=F32) / head)
        angles = positions.astype(F32)[..., None] * inv_freq
        cos, sin = jnp.cos(angles), jnp.sin(angles)
        top = max(dim, head)
        g_all = jnp.stack([jnp.pad(g.astype(F32), (0, top - g.shape[0]))
                           for g in (g_attn_in, g_attn_out, g_mlp_in, g_mlp_out, g_query, g_key)])
        pos_prev = lax.ppermute(positions, "cp", to_next)
        pos_prev = jnp.where(shard_idx > 0, pos_prev, -(2 ** 30))
        pos_ext = jnp.concatenate([pos_prev, positions], axis=1)[:, None, :]
        cs = per_seq(cos.shape)

        (kv,) = call(kv_kernel, n_batch, [x, cos, sin, w_key, w_value, g_all],
                     [per_seq(x.shape), cs, cs, whole(w_key.shape), whole(w_value.shape), whole(g_all.shape)],
                     [sds((n_batch, tokens, kv_dim), BF16)], [per_seq((n_batch, tokens, kv_dim))], [], 2 * n_tok * dim * kv_dim)

        stack = (n_batch, chunks, heads * qc, head)
        weights = [w_query, w_out, w_gate, w_up, w_down, g_all]
        lse_shape = (n_batch, chunks, 1, heads * qc)
        xs = per_seq(x.shape)
        y, d_mid, q_st, qp_st, da_st, lse, big, kv_prev, dg_main = call(
            functools.partial(main_kernel, window, scale, 512), n_batch,
            [x, dy, kv, cos, sin, pos_ext, kv] + weights,
            [xs, xs, per_seq(kv.shape), cs, cs, per_seq(pos_ext.shape), ANY] + [whole(w.shape) for w in weights],
            [sds(x.shape, BF16), sds(x.shape, F32), sds(stack, BF16), sds(stack, F32), sds(stack, BF16), sds(lse_shape, F32),
             sds((dim, wide), F32), sds(kv.shape, BF16), sds((8, dim), F32)],
            [xs, xs, per_seq(stack), per_seq(stack, pipeline_mode=pl.Buffered(1)), per_seq(stack), per_seq(lse_shape),
             ANY, ANY, whole((8, dim))],
            [pltpu.VMEM((dim, ffn), F32)] * 3 + [pltpu.VMEM((dim, q_dim), F32)]
            + [pltpu.VMEM((tokens, ffn), F32)] * 2 + [pltpu.VMEM((tokens, ffn), BF16), pltpu.VMEM((tokens, q_dim), BF16),
                                                     pltpu.VMEM((2, tokens, kv_dim), BF16),
                                                     dma((4,)), dma((2,)), dma((n_batch,)), dma((n_batch,))],
            2 * n_tok * (9 * dim * ffn + 4 * dim * q_dim + 2 * q_dim * keys),
            collective_id=0, has_side_effects=True)

        big = big.reshape(2, chips, slab, wide)
        part = (slab, max(piece_widths(wide)))
        first, behind = (lambda a: per_seq(a.shape, 0)), (lambda a: per_seq(a.shape, 1))
        seq_in = [kv, kv_prev, cos, sin, pos_ext, q_st, qp_st, da_st, lse]
        lag_in = [x, d_mid, cos, sin]
        back_w = [w_query, w_key, w_value, g_all]
        dw_shape = (dim, q_dim + kv_dim)
        dx, dw, dgi, dgq, dgk, full, _ = call(
            functools.partial(back_kernel, window, scale, n_batch), n_batch + 1,
            seq_in + lag_in + [big] + back_w,
            [first(a) for a in seq_in] + [behind(a) for a in lag_in] + [ANY] + [whole(w.shape) for w in back_w],
            [sds(x.shape, BF16), sds(dw_shape, F32), sds((1, dim), F32), sds((1, head), F32), sds((1, head), F32),
             sds(big.shape, BF16), sds(big.shape[1:], F32)],
            [behind(x), whole(dw_shape), whole((1, dim)), whole((1, head)), whole((1, head)), ANY, ANY],
            [pltpu.VMEM((keys, heads * qc), BF16)] * 2
            + [pltpu.VMEM((window + tokens, kv_dim), F32), pltpu.VMEM((2, tokens, q_dim + kv_dim), BF16),
               pltpu.VMEM((2, tokens, kv_dim), F32), pltpu.VMEM((2, window, kv_dim), BF16),
               pltpu.VMEM((n_batch, window, kv_dim), BF16), dma((2, 2)), dma((n_batch, 2))]
            + [pltpu.VMEM((2, 2, 2) + part, F32), pltpu.VMEM((2, 2) + part, BF16),
               pltpu.VMEM((2, chips - 1) + part, BF16), pltpu.VMEM((2,) + part, BF16),
               dma((2, chips)), dma((2, chips)), dma((2, 2, 2)), dma((2, chips - 1)), dma((2, chips - 1)),
               dma((2, chips - 1)), dma((2, chips - 1)), dma((2, chips)), dma((2, chips)), dma((2,))] * 2,
            2 * n_tok * (2 * dim * (q_dim + kv_dim) + 5 * q_dim * keys),
            collective_id=1, has_side_effects=True)

        full = full.reshape(dim, wide)
        r_dw, r_dg, r_dgq, r_dgi, r_dgk = lax.psum((dw, dg_main, dgq, dgi, dgk), "cp")
        b16 = lambda v: v.astype(BF16)
        kv_half = q_dim + kv_dim // 2
        return (y, dx, b16(r_dw[:, :q_dim]), b16(r_dw[:, q_dim:kv_half]), b16(r_dw[:, kv_half:]), full[:, 3 * ffn:].T,
                full[:, :ffn], full[:, ffn:2 * ffn], full[:, 2 * ffn:3 * ffn].T,
                b16(r_dgi[0]), b16(r_dg[2]), b16(r_dg[1]), b16(r_dg[0]), b16(r_dgq[0]), b16(r_dgk[0]))

    seq_spec = P("dp", "cp", None)
    in_specs = (seq_spec, seq_spec, P("dp", "cp")) + (P(None, None),) * 7 + (P(None),) * 6
    out_specs = (seq_spec, seq_spec) + (P("dp", None),) * 7 + (P("dp"),) * 6
    return jax.shard_map(local_step, mesh=mesh, in_specs=in_specs, out_specs=out_specs, check_vma=False)
```
